32 devices in a mesh: chan: 2 (over y), row: 8 (over z, x), col: 2 (over core).
Axes of the slice: x: 2, y: 2, z: 4, core: 2. Of those that a mesh axis runs over, the one named last changes fastest.
Arguments:
- hamiltonian_rows: float32 [16, 2, 2, 65536], P('chan', 'col', None, 'row'), parts along dimension 0, may hold values from -2 to 2, as said below
- current_block: float32 [131072, 256], P(('chan', 'row', 'col')), parts along dimension 0, may hold values from -6 to 6
- correction_block: float32 [131072, 256], P(('chan', 'row', 'col')), parts along dimension 0, may hold values from -6 to 6
- previous_block: float32 [131072, 256], P(('chan', 'row', 'col')), parts along dimension 0, may hold values from -6 to 6
- ritz_values: float32 [512], P('chan'), parts along dimension 0, may hold values from -2 to 2
- mixing_coeffs: float32 [1536, 256], P('chan'), parts along dimension 0, may hold values from -0.21875 to 0.21875
Outputs:
- next_block: float32 [64, 256], P(('chan', 'row', 'col')), parts along dimension 0
- next_direction: float32 [64, 256], P(('chan', 'row', 'col')), parts along dimension 0
- next_correction: float32 [64, 256], P(('chan', 'row', 'col')), parts along dimension 0
- ritz_matrix: float32 [512, 256], P('chan'), parts along dimension 0
- metric_matrix: float32 [512, 256], P('chan'), parts along dimension 0
The draws below stay inside these ranges and needn't reach their ends.
There are 2 independent parts, one for each index of `chan`. The reference program is written for one: setup_inputs(seed, part) draws one part's arguments, and reference() takes and returns one part's arrays. A program takes and returns all parts, laid end to end along the dimension named above; each array names one. Nothing has to cross between parts.
Inputs may be any that keep to these rules, and one draw needn't show every extreme that they name: hamiltonian_rows[a, b, j, :] is row (a * 2 + b) * 4096 + j of the channel's Hamiltonian; its entry in that row's own column is the onsite energy.
All inputs are finite; a program needn't handle non-finite values.
Results may differ from the reference program's by a relative error of at most 0.00008.
Values sent between devices are 32-bit elements; how exact they have to be, the bound alone decides.
A program may use at most 128 MiB of HBM per device.

```python
import math
import jax
import jax.numpy as jnp
from jax import lax

N = 65536
BLOCK = 256
OUT_DEV = 2
N_ROW = 8
N_COL = 2


def draw_hamiltonian_rows(key, part):
    first_key = jax.random.fold_in(key, 11)
    second_key = jax.random.fold_in(key, 12)
    shape = (N_ROW, N_COL, OUT_DEV, N)
    coupling = jax.random.truncated_normal(first_key, -6.0, 6.0, shape, jnp.float32) / math.sqrt(N)
    block_index = lax.broadcasted_iota(jnp.int32, shape, 0) * N_COL + lax.broadcasted_iota(jnp.int32, shape, 1)
    slot_index = lax.broadcasted_iota(jnp.int32, shape, 2)
    column_index = lax.broadcasted_iota(jnp.int32, shape, 3)
    position = (block_index * OUT_DEV + slot_index).astype(jnp.float32) / (N_ROW * N_COL * OUT_DEV)
    row_scale = jnp.exp(position * math.log(3.0))
    onsite = jax.random.uniform(second_key, (N_ROW, N_COL, OUT_DEV, 1), jnp.float32, -2.0, 2.0)
    own_column = column_index == block_index * (N // (N_ROW * N_COL)) + slot_index
    return jnp.where(own_column, onsite, coupling * row_scale)


def block_scale(rng, dims, cuts, smallest, largest):
    def one(dim, blocks):
        heights = jax.random.uniform(jax.random.fold_in(jax.random.fold_in(rng, 6), dim), (blocks,), jnp.float32, smallest / len(cuts), largest / len(cuts))
        return jnp.repeat(jnp.exp(heights), dims[dim] // blocks).reshape((-1,) + (1,) * (len(dims) - dim - 1))

    factor_of = one(*cuts[0])
    for cut in cuts[1:]:
        factor_of = factor_of * one(*cut)
    return factor_of


def normal_values(rng, shape, deviation, limit, cuts=(), held_as=jnp.bfloat16):
    entries = deviation * jax.random.normal(rng, shape, jnp.float32)
    if cuts:
        entries = entries * block_scale(rng, shape, cuts, -0.22, 0.18)
    return jnp.clip(entries, -limit, limit).astype(held_as)


def setup_inputs(seed: int = 0, part: int = 0) -> dict:
    keys = jax.random.split(jax.random.key(seed), 7)
    own_keys = jax.random.split(jax.random.fold_in(keys[6], part), 7)
    return {
        "hamiltonian_rows": draw_hamiltonian_rows(jax.random.fold_in(jax.random.fold_in(keys[6], part), 71), part),
        "current_block": normal_values(own_keys[1], (N, BLOCK), 1.0, 6.0, ((0, 16),), jnp.float32),
        "correction_block": normal_values(own_keys[2], (N, BLOCK), 1.0, 6.0, ((0, 16),), jnp.float32),
        "previous_block": normal_values(own_keys[3], (N, BLOCK), 1.0, 6.0, ((0, 16),), jnp.float32),
        "ritz_values": jnp.clip(jax.random.uniform(own_keys[4], (BLOCK,), jnp.float32, -2.0, 2.0), -2.0, 2.0),
        "mixing_coeffs": normal_values(own_keys[5], (3 * BLOCK, BLOCK), (3 * BLOCK) ** -0.5, 0.21875, (), jnp.float32),
    }


def matmul(left, right):
    return jnp.dot(left, right, preferred_element_type=jnp.float32, precision=lax.Precision.HIGHEST)

def tmatmul(left, right):
    return lax.dot_general(left, right, (((0,), (0,)), ((), ())), preferred_element_type=jnp.float32, precision=lax.Precision.HIGHEST)

def reference(hamiltonian_rows, current_block, correction_block, previous_block, ritz_values, mixing_coeffs):
    blocks = N_ROW * N_COL
    shard_rows = N // blocks
    whole_basis = jnp.concatenate([current_block, correction_block, previous_block], axis=1)
    window_rows = whole_basis.reshape(blocks, shard_rows, 3 * BLOCK)[:, :OUT_DEV, :].reshape(blocks * OUT_DEV, 3 * BLOCK)
    row_tile = hamiltonian_rows.reshape(blocks * OUT_DEV, N)
    product_rows = matmul(row_tile, whole_basis)
    residual = product_rows[:, :BLOCK] - window_rows[:, :BLOCK] * ritz_values[None, :]
    squares = lax.optimization_barrier(jnp.sum(residual * residual, axis=0))
    next_correction = residual * lax.rsqrt(squares / (blocks * OUT_DEV) + 1e-06)
    gram_basis = tmatmul(window_rows, window_rows)
    gram_product = tmatmul(window_rows, product_rows)
    next_block = matmul(window_rows, mixing_coeffs)
    next_direction = matmul(window_rows[:, BLOCK:], mixing_coeffs[BLOCK:, :])
    ritz_matrix = tmatmul(mixing_coeffs, matmul(gram_product, mixing_coeffs))
    metric_matrix = tmatmul(mixing_coeffs, matmul(gram_basis, mixing_coeffs))
    return (next_block, next_direction, next_correction, ritz_matrix, metric_matrix)
```

```python
import functools

import jax
import jax.numpy as jnp
from jax import lax
from jax.experimental import pallas as pl
from jax.experimental.pallas import tpu as pltpu
from jax.sharding import PartitionSpec as P

MESH = pl.DeviceIdType.MESH
F32 = jnp.float32
BF16 = jnp.bfloat16


def split(x):
    hi = x.astype(BF16)
    return hi, (x - hi.astype(F32)).astype(BF16)


def stack(x):
    return jnp.concatenate(split(x), axis=0)


def dot(a, b):
    return jnp.dot(a, b, preferred_element_type=F32)


def fold(x):
    half = x.shape[0] // 2
    return x[:half] + x[half:]


def tdot(at, b):
    return lax.dot_general(at, b, (((0,), (0,)), ((), ())), preferred_element_type=F32)


def kernel(
    n_row, n_col, chunks,
    h_ref, x_ref, w_ref, p_ref, ritz_ref, mix_ref,
    nb_out, nd_out, nc_out, rm_out, mm_out,
    hbuf, hsend, hf, hst, base, bhi, blo, top, mixf, mhi, mlo, ritz_v, acc,
    nb_all, rs_send, rs_recv, ag_all, nb_f, zm_f,
    base_sem, top_sem, mix_sem, ritz_sem, own_sem, stage_sem,
    h_sems, nb_sems, rs_sems, ag_sems,
):
    n = n_row * n_col
    row, col = lax.axis_index("row"), lax.axis_index("col")
    me = row * n_col + col
    blocks = (x_ref, w_ref, p_ref)
    out_rows = h_ref.shape[2]
    local, width = x_ref.shape
    step = local // chunks
    win = n * out_rows
    unroll = n <= 32

    def peers(body):
        def one(i, carry):
            p = lax.rem(me + i, n)
            body(p, {"row": p // n_col, "col": lax.rem(p, n_col)})
            return carry
        lax.fori_loop(1, n, one, 0, unroll=unroll)

    def cols(c):
        return pl.ds(pl.multiple_of(c * local, 128), local)

    def partner(i):
        return lax.rem(col + i, n_col)

    def stage(i):
        return pltpu.make_async_copy(h_ref.at[:, 0, :, cols(partner(i))], hsend.at[i - 1], stage_sem.at[i - 1])

    own = pltpu.make_async_copy(h_ref.at[:, 0, :, cols(col)], hbuf.at[col], own_sem)
    mix_copy = pltpu.make_async_copy(mix_ref, mixf, mix_sem)
    ritz_copy = pltpu.make_async_copy(ritz_ref, ritz_v, ritz_sem)

    def top_copy(b):
        return pltpu.make_async_copy(blocks[b].at[pl.ds(0, 8), :], top.at[b], top_sem.at[b])

    def base_copy(b, k):
        rows = pl.ds(pl.multiple_of(k * step, 8), step)
        return pltpu.make_async_copy(blocks[b].at[rows, :], base.at[b, rows, :], base_sem.at[b, k])

    for i in range(1, n_col):
        stage(i).start()
    for b in range(3):
        top_copy(b).start()
    mix_copy.start()
    own.start()
    ritz_copy.start()

    def start_base(k, carry):
        for b in range(3):
            base_copy(b, k).start()
        return carry
    lax.fori_loop(0, chunks, start_base, 0)

    barrier = pltpu.get_barrier_semaphore()
    peers(lambda p, dev: pl.semaphore_signal(barrier, inc=1, device_id=dev, device_id_type=MESH))

    for b in range(3):
        top_copy(b).wait()
    mix_copy.wait()
    hi, lo = split(mixf[...])
    mhi[...] = hi
    mlo[...] = lo
    lhs = [stack(top[b]) for b in range(3)]

    def part(b):
        rows = pl.ds(b * width, width)
        return fold(dot(lhs[b], mhi[rows, :]) + dot(lhs[b], mlo[rows, :]))
    nd = part(1) + part(2)
    nb = part(0) + nd
    nb_out[...] = nb[:out_rows]
    nd_out[...] = nd[:out_rows]
    nb_all[me] = nb[:out_rows]

    def cast(k, carry):
        rows = pl.ds(pl.multiple_of(k * step, 16), step)
        for b in range(3):
            base_copy(b, k).wait()
            hi, lo = split(base[b, rows, :])
            bhi[rows, pl.ds(b * width, width)] = hi
            blo[rows, pl.ds(b * width, width)] = lo
        return carry
    early = chunks // 2
    lax.fori_loop(0, early, cast, 0)

    for i in range(1, n_col):
        stage(i).wait()
    pl.semaphore_wait(barrier, n - 1)

    def h_copy(i):
        return pltpu.make_async_remote_copy(
            src_ref=hsend.at[i - 1], dst_ref=hbuf.at[col],
            send_sem=h_sems.at[0, i - 1], recv_sem=h_sems.at[1, i - 1],
            device_id={"row": row, "col": partner(i)}, device_id_type=MESH)
    for i in range(1, n_col):
        h_copy(i).start()

    def spread(src, dst, sems):
        def one(p, dev):
            pltpu.make_async_remote_copy(
                src_ref=src(p), dst_ref=dst.at[me], send_sem=sems.at[0], recv_sem=sems.at[1],
                device_id=dev, device_id_type=MESH).start()
        peers(one)

    def gather_wait(buf, sems, which):
        view = buf.at[pl.ds(0, n - 1)]
        pltpu.make_async_copy(view, view, sems.at[which]).wait()

    spread(lambda p: nb_all.at[me], nb_all, nb_sems)
    lax.fori_loop(early, chunks, cast, 0)

    own.wait()
    for i in range(1, n_col):
        h_copy(i).wait()
    for c in range(n_col):
        for a in range(n_row):
            at = (c * n_row + a) * out_rows
            hf[at:at + out_rows, :] = hbuf[c, a]
    hi, lo = split(hf[...])
    hst[:win, :] = hi
    hst[win:, :] = lo

    acc[...] = jnp.zeros_like(acc)

    def multiply(k, carry):
        rows = pl.ds(pl.multiple_of(k * step, 128), step)
        left = hst[:, rows]
        acc[...] += dot(left, bhi[rows, :]) + dot(left, blo[rows, :])
        return carry
    lax.fori_loop(0, chunks, multiply, 0)

    product = fold(acc[...])
    lhs2 = stack(product)
    mixed = fold(dot(lhs2, mhi[...]) + dot(lhs2, mlo[...]))
    for a in range(n_row):
        for c in range(n_col):
            at = (c * n_row + a) * out_rows
            rs_send[a * n_col + c, :, :width] = product[at:at + out_rows, :width]
            rs_send[a * n_col + c, :, width:] = mixed[at:at + out_rows]
    spread(lambda p: rs_send.at[p], rs_recv, rs_sems)
    rs_recv[me] = rs_send[me]

    gather_wait(nb_all, nb_sems, 1)
    for q in range(n):
        nb_f[q * out_rows:(q + 1) * out_rows, :] = nb_all[q]
    hi, lo = split(nb_f[...])
    left = jnp.concatenate([hi, hi, lo, lo], axis=0)
    mm_out[...] = tdot(left, jnp.concatenate([hi, lo, hi, lo], axis=0))
    ritz_copy.wait()

    gather_wait(rs_recv, rs_sems, 1)
    total = jnp.sum(rs_recv[...], axis=0)
    residual = total[:, :width] - top[0, :out_rows, :] * ritz_v[...]
    ag_all[me, :out_rows, :] = total[:, width:]
    ag_all[me, out_rows:out_rows + 1, :] = jnp.sum(residual * residual, axis=0, keepdims=True)
    spread(lambda p: ag_all.at[me], ag_all, ag_sems)

    gather_wait(ag_all, ag_sems, 1)
    squares = jnp.sum(ag_all[:, out_rows:out_rows + 1, :], axis=0)
    nc_out[...] = residual * lax.rsqrt(squares / win + 1e-6)
    for q in range(n):
        zm_f[q * out_rows:(q + 1) * out_rows, :] = ag_all[q, :out_rows, :]
    hi, lo = split(zm_f[...])
    rm_out[...] = tdot(left, jnp.concatenate([hi, lo, hi, lo], axis=0))
    gather_wait(nb_all, nb_sems, 0)
    gather_wait(rs_send, rs_sems, 0)
    gather_wait(ag_all, ag_sems, 0)


def solution(mesh):
    n_row, n_col = mesh.shape["row"], mesh.shape["col"]
    n = n_row * n_col

    def on_device(h, x, w, p, ritz, mix):
        local, width = x.shape
        out_rows = h.shape[2]
        win = n * out_rows
        chunks = max(local // 512, 2)
        vm = pltpu.VMEM
        dma = pltpu.SemaphoreType.DMA
        any_spec = pl.BlockSpec(memory_space=pl.ANY)
        vmem_spec = pl.BlockSpec(memory_space=pltpu.VMEM)
        return pl.pallas_call(
            functools.partial(kernel, n_row, n_col, chunks),
            out_shape=[jax.ShapeDtypeStruct((out_rows, width), F32)] * 3
            + [jax.ShapeDtypeStruct((width, width), F32)] * 2,
            in_specs=[any_spec] * 6,
            out_specs=[vmem_spec] * 5,
            scratch_shapes=[
                vm((n_col, n_row, out_rows, local), F32),
                vm((n_col - 1, n_row, out_rows, local), F32),
                vm((win, local), F32),
                vm((2 * win, local), BF16),
                vm((3, local, width), F32),
                vm((local, 3 * width), BF16),
                vm((local, 3 * width), BF16),
                vm((3, 8, width), F32),
                vm((3 * width, width), F32),
                vm((3 * width, width), BF16),
                vm((3 * width, width), BF16),
                vm((1, width), F32),
                vm((2 * win, 3 * width), F32),
                vm((n, out_rows, width), F32),
                vm((n, out_rows, 2 * width), F32),
                vm((n, out_rows, 2 * width), F32),
                vm((n, 2 * out_rows, width), F32),
                vm((win, width), F32),
                vm((win, width), F32),
                dma((3, chunks)), dma((3,)), dma, dma, dma, dma((n_col - 1,)),
                dma((2, n_col - 1)), dma((2,)), dma((2,)), dma((2,)),
            ],
            compiler_params=pltpu.CompilerParams(
                collective_id=0, has_side_effects=True, vmem_limit_bytes=60 * 1024 * 1024
            ),
        )(h, x, w, p, ritz.reshape(1, width), mix)

    blocks = P(("chan", "row", "col"), None)
    return jax.shard_map(
        on_device,
        mesh=mesh,
        in_specs=(P("chan", "col", None, "row"), blocks, blocks, blocks, P("chan"), P("chan", None)),
        out_specs=(blocks, blocks, blocks, P("chan", None), P("chan", None)),
        check_vma=False,
    )
```

```python
import functools

import jax
import jax.numpy as jnp
from jax import lax
from jax.experimental import pallas as pl
from jax.experimental.pallas import tpu as pltpu
from jax.sharding import PartitionSpec as P

MESH = pl.DeviceIdType.MESH
F32 = jnp.float32
BF16 = jnp.bfloat16


def split(x):
    hi = x.astype(BF16)
    return hi, (x - hi.astype(F32)).astype(BF16)


def stack(x):
    return jnp.concatenate(split(x), axis=0)


def dot(a, b):
    return jnp.dot(a, b, preferred_element_type=F32)


def fold(x):
    half = x.shape[0] // 2
    return x[:half] + x[half:]


def tdot(at, b):
    return lax.dot_general(at, b, (((0,), (0,)), ((), ())), preferred_element_type=F32)


def kernel(
    n_row, n_col, chunks,
    h_ref, x_ref, w_ref, p_ref, ritz_ref, mix_ref,
    small_out, rows_out,
    hbuf, hsend, hf, hst, base, bhi, blo, top, mixf, mhi, mlo, ritz_v, acc,
    nb_all, rs_send, rs_recv, ag_all,
    base_sem, top_sem, mix_sem, ritz_sem, own_sem, stage_sem,
    h_sems, nb_sems, rs_sems, ag_sems,
):
    n = n_row * n_col
    row, col = lax.axis_index("row"), lax.axis_index("col")
    me = row * n_col + col
    blocks = (x_ref, w_ref, p_ref)
    out_rows = h_ref.shape[2]
    local, width = x_ref.shape
    step = local // chunks
    win = n * out_rows
    unroll = n <= 32

    def peers(body):
        def one(i, carry):
            p = lax.rem(me + i, n)
            body(p, {"row": p // n_col, "col": lax.rem(p, n_col)})
            return carry
        lax.fori_loop(1, n, one, 0, unroll=unroll)

    def cols(c):
        return pl.ds(pl.multiple_of(c * local, 128), local)

    def partner(i):
        return lax.rem(col + i, n_col)

    def stage(i):
        return pltpu.make_async_copy(h_ref.at[:, 0, :, cols(partner(i))], hsend.at[i - 1], stage_sem.at[i - 1])

    own = pltpu.make_async_copy(h_ref.at[:, 0, :, cols(col)], hbuf.at[col], own_sem)
    mix_copy = pltpu.make_async_copy(mix_ref, mixf, mix_sem)
    ritz_copy = pltpu.make_async_copy(ritz_ref, ritz_v, ritz_sem)

    def top_copy(b):
        return pltpu.make_async_copy(blocks[b].at[pl.ds(0, 8), :], top.at[b], top_sem.at[b])

    def base_copy(b, k):
        rows = pl.ds(pl.multiple_of(k * step, 8), step)
        return pltpu.make_async_copy(blocks[b].at[rows, :], base.at[b, rows, :], base_sem.at[b, k])

    for i in range(1, n_col):
        stage(i).start()
    for b in range(3):
        top_copy(b).start()
    mix_copy.start()
    own.start()
    ritz_copy.start()

    def start_base(k, carry):
        for b in range(3):
            base_copy(b, k).start()
        return carry
    lax.fori_loop(0, chunks, start_base, 0)

    barrier = pltpu.get_barrier_semaphore()
    peers(lambda p, dev: pl.semaphore_signal(barrier, inc=1, device_id=dev, device_id_type=MESH))

    for b in range(3):
        top_copy(b).wait()
    mix_copy.wait()
    hi, lo = split(mixf[...])
    mhi[...] = hi
    mlo[...] = lo
    lhs = [stack(top[b]) for b in range(3)]

    def part(b):
        rows = pl.ds(b * width, width)
        return fold(dot(lhs[b], mhi[rows, :]) + dot(lhs[b], mlo[rows, :]))
    nd = part(1) + part(2)
    nb = part(0) + nd
    small_out[0] = nb[:out_rows]
    small_out[1] = nd[:out_rows]
    nb_all[me] = nb[:out_rows]

    def cast(k, carry):
        rows = pl.ds(pl.multiple_of(k * step, 16), step)
        for b in range(3):
            base_copy(b, k).wait()
            hi, lo = split(base[b, rows, :])
            bhi[rows, pl.ds(b * width, width)] = hi
            blo[rows, pl.ds(b * width, width)] = lo
        return carry
    early = chunks // 2
    lax.fori_loop(0, early, cast, 0)

    for i in range(1, n_col):
        stage(i).wait()
    pl.semaphore_wait(barrier, n - 1)

    def h_copy(i):
        return pltpu.make_async_remote_copy(
            src_ref=hsend.at[i - 1], dst_ref=hbuf.at[col],
            send_sem=h_sems.at[0, i - 1], recv_sem=h_sems.at[1, i - 1],
            device_id={"row": row, "col": partner(i)}, device_id_type=MESH)
    for i in range(1, n_col):
        h_copy(i).start()

    def spread(src, dst, sems):
        def one(p, dev):
            pltpu.make_async_remote_copy(
                src_ref=src(p), dst_ref=dst.at[me], send_sem=sems.at[0], recv_sem=sems.at[1],
                device_id=dev, device_id_type=MESH).start()
        peers(one)

    def gather_wait(buf, sems, which):
        view = buf.at[pl.ds(0, n - 1)]
        pltpu.make_async_copy(view, view, sems.at[which]).wait()

    spread(lambda p: nb_all.at[me], nb_all, nb_sems)
    lax.fori_loop(early, chunks, cast, 0)

    own.wait()
    for i in range(1, n_col):
        h_copy(i).wait()
    for c in range(n_col):
        for a in range(n_row):
            at = (c * n_row + a) * out_rows
            hf[at:at + out_rows, :] = hbuf[c, a]
    hi, lo = split(hf[...])
    hst[:win, :] = hi
    hst[win:, :] = lo

    acc[...] = jnp.zeros_like(acc)

    def multiply(k, carry):
        rows = pl.ds(pl.multiple_of(k * step, 128), step)
        left = hst[:, rows]
        acc[...] += dot(left, bhi[rows, :]) + dot(left, blo[rows, :])
        return carry
    lax.fori_loop(0, chunks, multiply, 0)

    product = fold(acc[...])
    lhs2 = stack(product)
    mixed = fold(dot(lhs2, mhi[...]) + dot(lhs2, mlo[...]))
    for a in range(n_row):
        for c in range(n_col):
            at = (c * n_row + a) * out_rows
            rs_send[a * n_col + c, :, :width] = product[at:at + out_rows, :width]
            rs_send[a * n_col + c, :, width:] = mixed[at:at + out_rows]
    spread(lambda p: rs_send.at[p], rs_recv, rs_sems)
    rs_recv[me] = rs_send[me]

    gather_wait(nb_all, nb_sems, 1)
    for q in range(n):
        rows_out[0, q * out_rows:(q + 1) * out_rows, :] = nb_all[q]
    ritz_copy.wait()

    gather_wait(rs_recv, rs_sems, 1)
    total = jnp.sum(rs_recv[...], axis=0)
    residual = total[:, :width] - top[0, :out_rows, :] * ritz_v[...]
    ag_all[me, :out_rows, :] = total[:, width:]
    ag_all[me, out_rows:out_rows + 1, :] = jnp.sum(residual * residual, axis=0, keepdims=True)
    spread(lambda p: ag_all.at[me], ag_all, ag_sems)

    gather_wait(ag_all, ag_sems, 1)
    squares = jnp.sum(ag_all[:, out_rows:out_rows + 1, :], axis=0)
    small_out[2] = residual * lax.rsqrt(squares / win + 1e-6)
    for q in range(n):
        rows_out[1, q * out_rows:(q + 1) * out_rows, :] = ag_all[q, :out_rows, :]
    gather_wait(nb_all, nb_sems, 0)
    gather_wait(rs_send, rs_sems, 0)
    gather_wait(ag_all, ag_sems, 0)


def finish(small, rows, nb_out, nd_out, nc_out, rm_out, mm_out):
    nb_out[...] = small[0]
    nd_out[...] = small[1]
    nc_out[...] = small[2]
    hi, lo = split(rows[0])
    left = jnp.concatenate([hi, hi, lo, lo], axis=0)
    mm_out[...] = tdot(left, jnp.concatenate([hi, lo, hi, lo], axis=0))
    hi, lo = split(rows[1])
    rm_out[...] = tdot(left, jnp.concatenate([hi, lo, hi, lo], axis=0))


def solution(mesh):
    n_row, n_col = mesh.shape["row"], mesh.shape["col"]
    n = n_row * n_col

    def on_device(h, x, w, p, ritz, mix):
        local, width = x.shape
        out_rows = h.shape[2]
        win = n * out_rows
        chunks = max(local // 512, 2)
        vm = pltpu.VMEM
        dma = pltpu.SemaphoreType.DMA
        any_spec = pl.BlockSpec(memory_space=pl.ANY)
        vmem_spec = pl.BlockSpec(memory_space=pltpu.VMEM)
        small, rows = pl.pallas_call(
            functools.partial(kernel, n_row, n_col, chunks),
            out_shape=[vm((3, out_rows, width), F32), vm((2, win, width), F32)],
            in_specs=[any_spec] * 6,
            out_specs=[vmem_spec] * 2,
            scratch_shapes=[
                vm((n_col, n_row, out_rows, local), F32),
                vm((n_col - 1, n_row, out_rows, local), F32),
                vm((win, local), F32),
                vm((2 * win, local), BF16),
                vm((3, local, width), F32),
                vm((local, 3 * width), BF16),
                vm((local, 3 * width), BF16),
                vm((3, 8, width), F32),
                vm((3 * width, width), F32),
                vm((3 * width, width), BF16),
                vm((3 * width, width), BF16),
                vm((1, width), F32),
                vm((2 * win, 3 * width), F32),
                vm((n, out_rows, width), F32),
                vm((n, out_rows, 2 * width), F32),
                vm((n, out_rows, 2 * width), F32),
                vm((n, 2 * out_rows, width), F32),
                dma((3, chunks)), dma((3,)), dma, dma, dma, dma((n_col - 1,)),
                dma((2, n_col - 1)), dma((2,)), dma((2,)), dma((2,)),
            ],
            compiler_params=pltpu.CompilerParams(
                collective_id=0, has_side_effects=True, vmem_limit_bytes=60 * 1024 * 1024
            ),
        )(h, x, w, p, ritz.reshape(1, width), mix)
        return pl.pallas_call(
            finish,
            out_shape=[jax.ShapeDtypeStruct((out_rows, width), F32)] * 3
            + [jax.ShapeDtypeStruct((width, width), F32)] * 2,
            in_specs=[vmem_spec] * 2,
            out_specs=[vmem_spec] * 5,
            compiler_params=pltpu.CompilerParams(vmem_limit_bytes=16 * 1024 * 1024),
        )(small, rows)

    blocks = P(("chan", "row", "col"), None)
    return jax.shard_map(
        on_device,
        mesh=mesh,
        in_specs=(P("chan", "col", None, "row"), blocks, blocks, blocks, P("chan"), P("chan", None)),
        out_specs=(blocks, blocks, blocks, P("chan", None), P("chan", None)),
        check_vma=False,
    )
```

```python
import functools

import jax
import jax.numpy as jnp
from jax import lax
from jax.experimental import pallas as pl
from jax.experimental.pallas import tpu as pltpu
from jax.sharding import PartitionSpec as P

MESH = pl.DeviceIdType.MESH
F32 = jnp.float32
BF16 = jnp.bfloat16


def split(x):
    hi = x.astype(BF16)
    return hi, (x - hi.astype(F32)).astype(BF16)


def stack(x):
    return jnp.concatenate(split(x), axis=0)


def dot(a, b):
    return jnp.dot(a, b, preferred_element_type=F32)


def fold(x):
    half = x.shape[0] // 2
    return x[:half] + x[half:]


def tdot(at, b):
    return lax.dot_general(at, b, (((0,), (0,)), ((), ())), preferred_element_type=F32)


def kernel(
    n_row, n_col, chunks,
    h_ref, x_ref, w_ref, p_ref, ritz_ref, mix_ref,
    small_out, rows_out,
    hbuf, hsend, hf, hst, base, bhi, blo, top, mixf, mhi, mlo, ritz_v, acc,
    nb_all, xs_send, xs_recv, rs_send, rs_recv, sq_all, ag_all,
    base_sem, top_sem, mix_sem, ritz_sem, own_sem, stage_sem,
    h_sems, nb_sems, xs_sems, rs_sems, sq_sems, ag_sems,
):
    n = n_row * n_col
    row, col = lax.axis_index("row"), lax.axis_index("col")
    me = row * n_col + col
    blocks = (x_ref, w_ref, p_ref)
    out_rows = h_ref.shape[2]
    local, width = x_ref.shape
    step = local // chunks
    win = n * out_rows
    unroll = n <= 32

    def peers(body):
        def one(i, carry):
            p = lax.rem(me + i, n)
            body(p, {"row": p // n_col, "col": lax.rem(p, n_col)})
            return carry
        lax.fori_loop(1, n, one, 0, unroll=unroll)

    def cols(c):
        return pl.ds(pl.multiple_of(c * local, 128), local)

    def partner(i):
        return lax.rem(col + i, n_col)

    def stage(i):
        return pltpu.make_async_copy(h_ref.at[:, 0, :, cols(partner(i))], hsend.at[i - 1], stage_sem.at[i - 1])

    own = pltpu.make_async_copy(h_ref.at[:, 0, :, cols(col)], hbuf.at[col], own_sem)
    mix_copy = pltpu.make_async_copy(mix_ref, mixf, mix_sem)
    ritz_copy = pltpu.make_async_copy(ritz_ref, ritz_v, ritz_sem)

    def top_copy(b):
        return pltpu.make_async_copy(blocks[b].at[pl.ds(0, 8), :], top.at[b], top_sem.at[b])

    def base_copy(b, k):
        rows = pl.ds(pl.multiple_of(k * step, 8), step)
        return pltpu.make_async_copy(blocks[b].at[rows, :], base.at[b, rows, :], base_sem.at[b, k])

    for i in range(1, n_col):
        stage(i).start()
    for b in range(3):
        top_copy(b).start()
    mix_copy.start()
    own.start()
    ritz_copy.start()

    def start_base(k, carry):
        for b in range(3):
            base_copy(b, k).start()
        return carry
    lax.fori_loop(0, chunks, start_base, 0)

    barrier = pltpu.get_barrier_semaphore()
    peers(lambda p, dev: pl.semaphore_signal(barrier, inc=1, device_id=dev, device_id_type=MESH))

    for b in range(3):
        top_copy(b).wait()
    mix_copy.wait()
    hi, lo = split(mixf[...])
    mhi[...] = hi
    mlo[...] = lo
    lhs = [stack(top[b]) for b in range(3)]

    def part(b):
        rows = pl.ds(b * width, width)
        return fold(dot(lhs[b], mhi[rows, :]) + dot(lhs[b], mlo[rows, :]))
    nd = part(1) + part(2)
    nb = part(0) + nd
    small_out[0] = nb[:out_rows]
    small_out[1] = nd[:out_rows]
    nb_all[me] = nb[:out_rows]

    def cast(k, carry):
        rows = pl.ds(pl.multiple_of(k * step, 16), step)
        for b in range(3):
            base_copy(b, k).wait()
            hi, lo = split(base[b, rows, :])
            bhi[rows, pl.ds(b * width, width)] = hi
            blo[rows, pl.ds(b * width, width)] = lo
        return carry
    early = chunks // 2
    lax.fori_loop(0, early, cast, 0)

    for i in range(1, n_col):
        stage(i).wait()
    pl.semaphore_wait(barrier, n - 1)

    def h_copy(i):
        return pltpu.make_async_remote_copy(
            src_ref=hsend.at[i - 1], dst_ref=hbuf.at[col],
            send_sem=h_sems.at[0, i - 1], recv_sem=h_sems.at[1, i - 1],
            device_id={"row": row, "col": partner(i)}, device_id_type=MESH)
    for i in range(1, n_col):
        h_copy(i).start()

    def spread(src, dst, sems):
        def one(p, dev):
            pltpu.make_async_remote_copy(
                src_ref=src(p), dst_ref=dst.at[me], send_sem=sems.at[0], recv_sem=sems.at[1],
                device_id=dev, device_id_type=MESH).start()
        peers(one)

    def gather_wait(buf, sems, which):
        view = buf.at[pl.ds(0, n - 1)]
        pltpu.make_async_copy(view, view, sems.at[which]).wait()

    spread(lambda p: nb_all.at[me], nb_all, nb_sems)
    lax.fori_loop(early, chunks, cast, 0)

    own.wait()
    for i in range(1, n_col):
        h_copy(i).wait()
    for c in range(n_col):
        for a in range(n_row):
            at = (c * n_row + a) * out_rows
            hf[at:at + out_rows, :] = hbuf[c, a]
    hi, lo = split(hf[...])
    hst[:win, :] = hi
    hst[win:, :] = lo

    acc[...] = jnp.zeros_like(acc)

    def multiply(span):
        def one(k, carry):
            rows = pl.ds(pl.multiple_of(k * step, 128), step)
            left = hst[:, rows]
            acc[:, span] += dot(left, bhi[rows, span]) + dot(left, blo[rows, span])
            return carry
        lax.fori_loop(0, chunks, one, 0)
        return fold(acc[:, span])

    def scatter(value, send, recv, sems):
        for a in range(n_row):
            for c in range(n_col):
                at = (c * n_row + a) * out_rows
                send[a * n_col + c] = value[at:at + out_rows]
        spread(lambda p: send.at[p], recv, sems)
        recv[me] = send[me]

    product = multiply(slice(0, width))
    scatter(product, xs_send, xs_recv, xs_sems)
    product = jnp.concatenate([product, multiply(slice(width, 3 * width))], axis=1)
    lhs2 = stack(product)
    mixed = fold(dot(lhs2, mhi[...]) + dot(lhs2, mlo[...]))
    scatter(mixed, rs_send, rs_recv, rs_sems)

    ritz_copy.wait()
    gather_wait(xs_recv, xs_sems, 1)
    residual = jnp.sum(xs_recv[...], axis=0) - top[0, :out_rows, :] * ritz_v[...]
    sq_all[me] = jnp.sum(residual * residual, axis=0, keepdims=True)
    spread(lambda p: sq_all.at[me], sq_all, sq_sems)

    gather_wait(nb_all, nb_sems, 1)
    for q in range(n):
        rows_out[0, q * out_rows:(q + 1) * out_rows, :] = nb_all[q]

    gather_wait(rs_recv, rs_sems, 1)
    ag_all[me] = jnp.sum(rs_recv[...], axis=0)
    spread(lambda p: ag_all.at[me], ag_all, ag_sems)

    gather_wait(sq_all, sq_sems, 1)
    squares = jnp.sum(sq_all[...], axis=0)
    small_out[2] = residual * lax.rsqrt(squares / win + 1e-6)
    gather_wait(ag_all, ag_sems, 1)
    for q in range(n):
        rows_out[1, q * out_rows:(q + 1) * out_rows, :] = ag_all[q]
    gather_wait(nb_all, nb_sems, 0)
    gather_wait(xs_send, xs_sems, 0)
    gather_wait(rs_send, rs_sems, 0)
    gather_wait(sq_all, sq_sems, 0)
    gather_wait(ag_all, ag_sems, 0)


def finish(small, rows, nb_out, nd_out, nc_out, rm_out, mm_out):
    nb_out[...] = small[0]
    nd_out[...] = small[1]
    nc_out[...] = small[2]
    hi, lo = split(rows[0])
    left = jnp.concatenate([hi, hi, lo, lo], axis=0)
    mm_out[...] = tdot(left, jnp.concatenate([hi, lo, hi, lo], axis=0))
    hi, lo = split(rows[1])
    rm_out[...] = tdot(left, jnp.concatenate([hi, lo, hi, lo], axis=0))


def solution(mesh):
    n_row, n_col = mesh.shape["row"], mesh.shape["col"]
    n = n_row * n_col

    def on_device(h, x, w, p, ritz, mix):
        local, width = x.shape
        out_rows = h.shape[2]
        win = n * out_rows
        chunks = max(local // 512, 2)
        vm = pltpu.VMEM
        dma = pltpu.SemaphoreType.DMA
        any_spec = pl.BlockSpec(memory_space=pl.ANY)
        vmem_spec = pl.BlockSpec(memory_space=pltpu.VMEM)
        small, rows = pl.pallas_call(
            functools.partial(kernel, n_row, n_col, chunks),
            out_shape=[vm((3, out_rows, width), F32), vm((2, win, width), F32)],
            in_specs=[any_spec] * 6,
            out_specs=[vmem_spec] * 2,
            scratch_shapes=[
                vm((n_col, n_row, out_rows, local), F32),
                vm((n_col - 1, n_row, out_rows, local), F32),
                vm((win, local), F32),
                vm((2 * win, local), BF16),
                vm((3, local, width), F32),
                vm((local, 3 * width), BF16),
                vm((local, 3 * width), BF16),
                vm((3, 8, width), F32),
                vm((3 * width, width), F32),
                vm((3 * width, width), BF16),
                vm((3 * width, width), BF16),
                vm((1, width), F32),
                vm((2 * win, 3 * width), F32),
                vm((n, out_rows, width), F32),
                vm((n, out_rows, width), F32),
                vm((n, out_rows, width), F32),
                vm((n, out_rows, width), F32),
                vm((n, out_rows, width), F32),
                vm((n, 1, width), F32),
                vm((n, out_rows, width), F32),
                dma((3, chunks)), dma((3,)), dma, dma, dma, dma((n_col - 1,)),
                dma((2, n_col - 1)), dma((2,)), dma((2,)), dma((2,)), dma((2,)), dma((2,)),
            ],
            compiler_params=pltpu.CompilerParams(
                collective_id=0, has_side_effects=True, vmem_limit_bytes=60 * 1024 * 1024
            ),
        )(h, x, w, p, ritz.reshape(1, width), mix)
        return pl.pallas_call(
            finish,
            out_shape=[jax.ShapeDtypeStruct((out_rows, width), F32)] * 3
            + [jax.ShapeDtypeStruct((width, width), F32)] * 2,
            in_specs=[vmem_spec] * 2,
            out_specs=[vmem_spec] * 5,
            compiler_params=pltpu.CompilerParams(vmem_limit_bytes=16 * 1024 * 1024),
        )(small, rows)

    blocks = P(("chan", "row", "col"), None)
    return jax.shard_map(
        on_device,
        mesh=mesh,
        in_specs=(P("chan", "col", None, "row"), blocks, blocks, blocks, P("chan"), P("chan", None)),
        out_specs=(blocks, blocks, blocks, P("chan", None), P("chan", None)),
        check_vma=False,
    )
```
